32 devices in a mesh: node: 8 (over z, x), expert: 4 (over y, core).
Axes of the slice: x: 2, y: 2, z: 4, core: 2. Of those that a mesh axis runs over, the one named last changes fastest.
Arguments:
- param_gu: float32 [32768, 1024], P('node', 'expert'), may hold values from -13 to 13
- param_down: float32 [1024, 16384], P('node', 'expert'), may hold values from -13 to 13
- tokens: bfloat16 [4096, 4096], P(('node', 'expert')), may hold values from -6 to 6
- cotangent: bfloat16 [4096, 4096], P(('node', 'expert')), may hold values from -6 to 6
- routes: int32 [4096, 2], P(('node', 'expert')), may hold values from 0 to 3, all different within a row; in each aligned block of 128 rows (0 to 127, 128 to 255, ...) at most 96 rows name the same one
- plan: int32 [4], replicated, may hold values from 0 to 5
Outputs:
- gossiped_gu: bfloat16 [32768, 1024], P('node', 'expert')
- gossiped_down: bfloat16 [1024, 16384], P('node', 'expert')
- averaged_gu: float32 [4096, 1024], P('node', 'expert')
- averaged_down: float32 [128, 16384], P('node', 'expert')
The draws below stay inside these ranges and needn't reach their ends.
Inputs may be any that keep to these rules, and one draw needn't show every extreme that they name: `routes`: each row names 2 different experts; the rows of one device name one expert 96 times at most.
All inputs are finite; a program needn't handle non-finite values.
Results may differ from the reference program's by a relative error of at most 0.0078.
Values may be sent and summed in bfloat16 or wider, within the bound.
A program may use at most 128 MiB of HBM per device.

```python
import math
import jax
import jax.numpy as jnp
import numpy as np
from jax import lax

D = 4096
H = 128
TOK_DEV = 128
TOP = 2
ROUNDS = 4
SHIFTS = 6
CAP = 96
EXPERTS = 4
TOKENS = 4096
N_NODE = 8


def replica_field(key, per_node, columns):
    total = N_NODE * per_node
    replica = (jnp.arange(total, dtype=jnp.int32) // per_node).astype(jnp.float32)
    frac = (replica / max(N_NODE - 1, 1))[:, None]
    noise = jnp.clip(jax.random.normal(key, (total, columns), jnp.float32), -4.0, 4.0)
    scale = 1.0 + 2.0 * frac
    offset = frac - 0.5
    return scale * noise + offset


def draw_param_gu(key, part):
    return replica_field(jax.random.fold_in(key, 11), D, EXPERTS * 2 * H)


def draw_param_down(key, part):
    return replica_field(jax.random.fold_in(key, 23), H, EXPERTS * D)


def touch_ends(drawn, key, least, largest):
    spot = [jax.random.randint(jax.random.fold_in(key, axis), (), 0, length) for axis, length in enumerate(drawn.shape)]
    widest = drawn.shape.index(max(drawn.shape))
    next_to = spot[:widest] + [(spot[widest] + 1) % drawn.shape[widest]] + spot[widest + 1:]
    return drawn.at[tuple(spot)].set(least).at[tuple(next_to)].set(largest)


def levels(key, extent, pieces, smallest, top_value):
    gain = 1.0
    for axis_at, shards_of in pieces:
        draws = jax.random.uniform(jax.random.fold_in(jax.random.fold_in(key, 6), axis_at), (shards_of,), jnp.float32, smallest / len(pieces), top_value / len(pieces))
        gain = gain * jnp.repeat(jnp.exp(draws), extent[axis_at] // shards_of).reshape((-1,) + (1,) * (len(extent) - 1 - axis_at))
    return gain


def deal_out(stream_key, own, number, rows, number_of, top, most, skew):
    ranking = jax.random.permutation(stream_key, number_of)
    crowded, common = shares(number_of, rows * top, most, skew, True), shares(number_of, rows * top, most, skew, False)
    places = jnp.arange(number_of)

    def named(lengths, offset_by):
        used = int((lengths > 0).sum())
        fixed = max(1, used // 4)
        moved = fixed + (places - fixed + offset_by * (used - fixed)) % max(1, number_of - fixed)
        return jnp.zeros((number_of,), jnp.int32).at[ranking[jnp.where(places < fixed, places, moved)]].set(jnp.asarray(lengths, jnp.int32))

    lengths = jnp.where(number % 4 == 0, named(crowded, number // 4), named(common, number - number // 4 - 1))
    mixed = jax.random.permutation(jax.random.fold_in(own, 3), number_of)
    source_of, receiver = mixed[0:number_of // 2 * 2:2], mixed[1:number_of // 2 * 2:2]
    room = jnp.minimum(lengths[source_of] - 1, most - lengths[receiver]) // 2
    room = jnp.where((source_of == ranking[0]) | (receiver == ranking[0]) | (lengths[receiver] == 0), 0, jnp.maximum(room, 0))
    moved = jax.random.randint(jax.random.fold_in(own, 4), (number_of // 2,), 0, 1 << 20) % (room + 1)
    lengths = lengths.at[source_of].add(-moved).at[receiver].add(moved)
    items = jnp.searchsorted(jnp.cumsum(lengths), jnp.arange(rows * top), side="right").astype(jnp.int32)
    listing = items.reshape(top, rows).T
    listing = listing[jax.random.permutation(jax.random.fold_in(own, 1), rows)]
    offset_by = jax.random.randint(jax.random.fold_in(own, 2), (rows, 1), 0, top)
    return jnp.take_along_axis(listing, (jnp.arange(top)[None, :] + offset_by) % top, axis=1)


def shares(count, total, bound, lean, full):
    loads = [(1 << 20) // math.isqrt(rank ** lean) + 1 for rank in range(1, count + 1)]
    largest = bound if full else min(bound, max(-(-total // count), total * loads[0] // sum(loads)))
    least = 1 if total - largest >= count - 1 else 0
    counts, rest = [largest] + [least] * (count - 1), total - largest - least * (count - 1)
    while rest > 0:
        free = [i for i in range(1, count) if counts[i] < largest] or [i for i in range(1, count) if counts[i] < bound]
        whole, remaining = sum([loads[i] for i in free]), rest
        for i in free:
            addition = min(bound - counts[i], max(1, remaining * loads[i] // whole), rest)
            counts[i] = counts[i] + addition
            rest = rest - addition
    return np.array(counts)


def normal_values(key, dims, spread, bound, shards=(), held_as=jnp.bfloat16):
    level = levels(key, dims, shards, -0.22, 0.18) if shards else 1.0
    entries = jax.random.normal(key, dims, jnp.float32) * spread * level
    return jnp.minimum(jnp.maximum(entries, -bound), bound).astype(held_as)


def setup_inputs(seed: int = 0) -> dict:
    arg_keys = jax.random.split(jax.random.key(seed), 7)
    param_gu = draw_param_gu(jax.random.fold_in(arg_keys[6], 71), 0)
    param_down = draw_param_down(jax.random.fold_in(arg_keys[6], 71), 0)
    tokens = normal_values(arg_keys[2], (TOKENS, D), 1.0, 6.0, ((0, 32),))
    cotangent = normal_values(arg_keys[3], (TOKENS, D), 1.0, 6.0, ((0, 32),))
    routes_keys = jax.random.split(jax.random.fold_in(arg_keys[4], 1), TOKENS // TOK_DEV)
    routes_turns = jax.random.permutation(jax.random.fold_in(arg_keys[4], 3), TOKENS // TOK_DEV)
    routes = jax.vmap(lambda own, number: deal_out(jax.random.fold_in(arg_keys[4], 2), own, number, TOK_DEV, EXPERTS, TOP, CAP, 2))(routes_keys, routes_turns).reshape((TOKENS, TOP))
    plan = touch_ends(jax.random.randint(arg_keys[5], (ROUNDS,), 0, SHIFTS), jax.random.fold_in(arg_keys[5], 1), 0, SHIFTS - 1).astype(jnp.int32)
    return {"param_gu": param_gu, "param_down": param_down, "tokens": tokens, "cotangent": cotangent, "routes": routes, "plan": plan}


def expert_grads(rows, douts, wgu, wdown):
    hid = wdown.shape[0]
    width = rows.shape[1]
    both = jnp.dot(rows, wgu, preferred_element_type=jnp.float32) * (1.0 / math.sqrt(width))
    gate = both[:, :hid]
    upper = both[:, hid:]
    sigma = jax.nn.sigmoid(gate)
    act = (gate * sigma * upper).astype(jnp.bfloat16)
    dact = jnp.dot(douts, wdown.T, preferred_element_type=jnp.float32) * (1.0 / math.sqrt(hid))
    dgate = dact * upper * sigma * (1.0 + gate * (1.0 - sigma))
    dupper = dact * gate * sigma
    dboth = jnp.concatenate([dgate, dupper], axis=1).astype(jnp.bfloat16)
    grad_down = jnp.dot(act.T, douts, preferred_element_type=jnp.float32) * (1.0 / math.sqrt(hid))
    grad_gu = jnp.dot(rows.T, dboth, preferred_element_type=jnp.float32) * (1.0 / math.sqrt(width))
    return (grad_gu, grad_down)

def reference(param_gu, param_down, tokens, cotangent, routes, plan):
    nodes = N_NODE
    groups = EXPERTS
    hid = H
    width = D
    gu_all = param_gu.reshape(nodes, width, groups, 2 * hid)
    down_all = param_down.reshape(nodes, hid, groups, width)
    tok_all = tokens.reshape(nodes, -1, width)
    cot_all = cotangent.reshape(nodes, -1, width)
    route_all = routes.reshape(nodes, -1, TOP)

    def per_node(items):
        gu_node, down_node, inputs, douts, chosen = items
        new_gu = []
        new_down = []
        for expert in range(groups):
            picked = jnp.any(chosen == expert, axis=1)[:, None]
            rows = jnp.where(picked, inputs, jnp.zeros_like(inputs))
            drows = jnp.where(picked, douts, jnp.zeros_like(douts))
            grad_gu, grad_down = expert_grads(rows, drows, gu_node[:, expert].astype(jnp.bfloat16), down_node[:, expert].astype(jnp.bfloat16))
            new_gu.append(gu_node[:, expert] - 0.5 * grad_gu)
            new_down.append(down_node[:, expert] - 0.5 * grad_down)
        return (jnp.stack(new_gu, axis=1), jnp.stack(new_down, axis=1))
    state_gu, state_down = lax.map(per_node, (gu_all, down_all, tok_all, cot_all, route_all))
    ranks = jnp.arange(nodes, dtype=jnp.int32)
    for step in range(ROUNDS):
        shift_by = jnp.left_shift(jnp.int32(1), plan[step].astype(jnp.int32))
        peer = ((ranks + shift_by) % nodes).astype(jnp.int32)
        recv_gu = lax.optimization_barrier(state_gu[peer].astype(jnp.bfloat16)).astype(jnp.float32)
        recv_down = lax.optimization_barrier(state_down[peer].astype(jnp.bfloat16)).astype(jnp.float32)
        state_gu = (state_gu + recv_gu) * 0.5
        state_down = (state_down + recv_down) * 0.5
    gossiped_gu = state_gu.astype(jnp.bfloat16).reshape(nodes * width, groups * 2 * hid)
    gossiped_down = state_down.astype(jnp.bfloat16).reshape(nodes * hid, groups * width)
    averaged_gu = (lax.optimization_barrier(jnp.sum(state_gu, axis=0)) / nodes).reshape(width, groups * 2 * hid)
    averaged_down = (lax.optimization_barrier(jnp.sum(state_down, axis=0)) / nodes).reshape(hid, groups * width)
    return (gossiped_gu, gossiped_down, averaged_gu, averaged_down)
```

```python
import math

import jax
import jax.numpy as jnp
from jax import lax
from jax.sharding import PartitionSpec as P


def everyone(value, axis):
    count = lax.axis_size(axis)
    spread = jnp.broadcast_to(value[None], (count,) + value.shape)
    return lax.all_to_all(spread, axis, 0, 0)


def body(param_gu, param_down, tokens, cotangent, routes, plan):
    nodes = lax.axis_size("node")
    width = tokens.shape[1]
    hid = param_down.shape[0]
    mine = lax.axis_index("expert")
    rows = everyone(tokens, "expert").reshape(-1, width)
    douts = everyone(cotangent, "expert").reshape(-1, width)
    chosen = lax.all_gather(routes, "expert", axis=0, tiled=True)
    picked = jnp.any(chosen == mine, axis=1)[:, None]
    wgu = param_gu.astype(jnp.bfloat16)
    wdown = param_down.astype(jnp.bfloat16)
    both = jnp.dot(rows, wgu, preferred_element_type=jnp.float32) * (1.0 / math.sqrt(width))
    gate = both[:, :hid]
    upper = both[:, hid:]
    sigma = jax.nn.sigmoid(gate)
    act = jnp.where(picked, gate * sigma * upper, 0.0).astype(jnp.bfloat16)
    dact = jnp.dot(douts, wdown.T, preferred_element_type=jnp.float32) * (1.0 / math.sqrt(hid))
    dgate = dact * upper * sigma * (1.0 + gate * (1.0 - sigma))
    dupper = dact * gate * sigma
    dboth = jnp.where(picked, jnp.concatenate([dgate, dupper], axis=1), 0.0).astype(jnp.bfloat16)
    grad_down = jnp.dot(act.T, douts, preferred_element_type=jnp.float32) * (1.0 / math.sqrt(hid))
    grad_gu = jnp.dot(rows.T, dboth, preferred_element_type=jnp.float32) * (1.0 / math.sqrt(width))
    state_gu = (param_gu - 0.5 * grad_gu).astype(jnp.bfloat16)
    state_down = (param_down - 0.5 * grad_down).astype(jnp.bfloat16)

    distance = jnp.left_shift(jnp.int32(1), plan) % nodes
    ranks = jnp.arange(nodes)
    mixing = jnp.eye(nodes, dtype=jnp.float32)
    for step in range(plan.shape[0]):
        mixing = 0.5 * (mixing + jnp.take(mixing, (ranks + distance[step]) % nodes, axis=0))

    def gossip(state):
        split = state.reshape(nodes, -1, state.shape[1])
        held = lax.all_to_all(split, "node", 0, 0)
        mean = jnp.mean(held.astype(jnp.float32), axis=0)
        mixed = jnp.einsum("nm,mrc->nrc", mixing.astype(jnp.bfloat16), held, preferred_element_type=jnp.float32)
        back = lax.all_to_all(mixed.astype(jnp.bfloat16), "node", 0, 0)
        return back.reshape(state.shape), mean

    gossiped_down, averaged_down = gossip(state_down)
    gossiped_gu, averaged_gu = gossip(state_gu)
    return (gossiped_gu, gossiped_down, averaged_gu, averaged_down)


def solution(mesh):
    both = P("node", "expert")
    rows = P(("node", "expert"), None)
    return jax.shard_map(body, mesh=mesh, in_specs=(both, both, rows, rows, rows, P()), out_specs=(both,) * 4, check_vma=False)
```

```python
from functools import partial
import math

import jax
import jax.numpy as jnp
from jax import lax
from jax.experimental import pallas as pl
from jax.experimental.pallas import tpu as pltpu
from jax.sharding import PartitionSpec as P


def everyone(value, axis):
    count = lax.axis_size(axis)
    spread = jnp.broadcast_to(value[None], (count,) + value.shape)
    return lax.all_to_all(spread, axis, 0, 0)


def plain_body(param_gu, param_down, tokens, cotangent, routes, plan):
    nodes = lax.axis_size("node")
    width = tokens.shape[1]
    hid = param_down.shape[0]
    mine = lax.axis_index("expert")
    rows = everyone(tokens, "expert").reshape(-1, width)
    douts = everyone(cotangent, "expert").reshape(-1, width)
    chosen = lax.all_gather(routes, "expert", axis=0, tiled=True)
    picked = jnp.any(chosen == mine, axis=1)[:, None]
    wgu = param_gu.astype(jnp.bfloat16)
    wdown = param_down.astype(jnp.bfloat16)
    both = jnp.dot(rows, wgu, preferred_element_type=jnp.float32) * (1.0 / math.sqrt(width))
    gate = both[:, :hid]
    upper = both[:, hid:]
    sigma = jax.nn.sigmoid(gate)
    act = jnp.where(picked, gate * sigma * upper, 0.0).astype(jnp.bfloat16)
    dact = jnp.dot(douts, wdown.T, preferred_element_type=jnp.float32) * (1.0 / math.sqrt(hid))
    dgate = dact * upper * sigma * (1.0 + gate * (1.0 - sigma))
    dupper = dact * gate * sigma
    dboth = jnp.where(picked, jnp.concatenate([dgate, dupper], axis=1), 0.0).astype(jnp.bfloat16)
    grad_down = jnp.dot(act.T, douts, preferred_element_type=jnp.float32) * (1.0 / math.sqrt(hid))
    grad_gu = jnp.dot(rows.T, dboth, preferred_element_type=jnp.float32) * (1.0 / math.sqrt(width))
    state_gu = (param_gu - 0.5 * grad_gu).astype(jnp.bfloat16)
    state_down = (param_down - 0.5 * grad_down).astype(jnp.bfloat16)

    distance = jnp.left_shift(jnp.int32(1), plan) % nodes
    ranks = jnp.arange(nodes)
    mixing = jnp.eye(nodes, dtype=jnp.float32)
    for step in range(plan.shape[0]):
        mixing = 0.5 * (mixing + jnp.take(mixing, (ranks + distance[step]) % nodes, axis=0))

    def gossip(state):
        split = state.reshape(nodes, -1, state.shape[1])
        held = lax.all_to_all(split, "node", 0, 0)
        mean = jnp.mean(held.astype(jnp.float32), axis=0)
        mixed = jnp.einsum("nm,mrc->nrc", mixing.astype(jnp.bfloat16), held, preferred_element_type=jnp.float32)
        back = lax.all_to_all(mixed.astype(jnp.bfloat16), "node", 0, 0)
        return back.reshape(state.shape), mean

    gossiped_down, averaged_down = gossip(state_down)
    gossiped_gu, averaged_gu = gossip(state_gu)
    return (gossiped_gu, gossiped_down, averaged_gu, averaged_down)


X_CHUNKS = 2
DY_CHUNKS = 4
GU_CHUNKS = 4
DOWN_CHUNKS = 2
MESH = pl.DeviceIdType.MESH


def mixing_of(plan, nodes):
    ranks = jnp.arange(nodes)
    mixing = jnp.eye(nodes, dtype=jnp.float32)
    distance = jnp.left_shift(jnp.int32(1), plan) % nodes
    for step in range(plan.shape[0]):
        shifted = (ranks[:, None] + distance[step]) % nodes == ranks[None, :]
        mixing = 0.5 * (mixing + jnp.dot(shifted.astype(jnp.float32), mixing, precision="highest"))
    return mixing


def kernel(nodes, mix_ref, gu_in, down_in, x_in, dy_in, pick_in, og_gu, og_down, avg_gu, avg_down,
           par_gu, par_down, xs, dys, xt, picks, wgu, wdown, both_s, act_s, dgu_s,
           p_gu, p_down, l_gu, l_down, t_gu, t_down, m_gu, m_down,
           loc_sem, tok_send, tok_recv, pick_send, pick_recv, a_send, a_recv):
    me = lax.axis_index("node")
    e = lax.axis_index("expert")
    deep = nodes // 2
    z, x = lax.div(me, 2), lax.rem(me, 2)
    partner = e + 1 - 2 * lax.rem(e, 2)
    cross = lax.rem(e + 2, 4)
    diag = partner + 2 - 4 * lax.div(partner, 2)
    tok, width = x_in.shape
    hid = down_in.shape[0]

    def node_at(dz, dx):
        return lax.rem(z + dz + deep, deep) * 2 + lax.rem(x + dx, 2)

    barrier = pltpu.get_barrier_semaphore()
    offsets = [(dz, dx) for dz in range(deep) for dx in range(2)][1:]
    for other in (partner, cross, diag):
        pl.semaphore_signal(barrier, inc=1, device_id={"expert": other}, device_id_type=MESH)
    for dz, dx in offsets:
        pl.semaphore_signal(barrier, inc=1, device_id={"node": node_at(dz, dx)}, device_id_type=MESH)

    local = [
        pltpu.make_async_copy(x_in, xs.at[0], loc_sem.at[0]),
        pltpu.make_async_copy(gu_in, par_gu, loc_sem.at[1]),
        pltpu.make_async_copy(down_in, par_down, loc_sem.at[2]),
        pltpu.make_async_copy(dy_in, dys.at[0], loc_sem.at[3]),
    ]
    for copy in local:
        copy.start()
    pl.semaphore_wait(barrier, 3 + len(offsets))

    def piece(which, k):
        if which == 0:
            size = tok // X_CHUNKS
            return (pl.ds(k * size, size), slice(None))
        size = width // DY_CHUNKS
        return (slice(None), pl.ds(k * size, size))

    def token_copy(which, k, route):
        part = piece(which, k)
        buf = (xs, dys)[which]
        at = (0 if which == 0 else X_CHUNKS) + k
        if route == 2:
            src = buf.at[(2,) + part]
        else:
            src = (x_in, dy_in)[which].at[part]
        return pltpu.make_async_remote_copy(
            src, buf.at[(route + 1,) + part], tok_send.at[at, route], tok_recv.at[at, route],
            device_id={"expert": cross if route == 1 else partner}, device_id_type=MESH)

    def pick_copy(i):
        return pltpu.make_async_remote_copy(
            pick_in, picks.at[i], pick_send.at[i], pick_recv.at[i],
            device_id={"expert": (partner, cross, diag)[i]}, device_id_type=MESH)

    order = [(0, k) for k in range(X_CHUNKS)] + [(1, k) for k in range(DY_CHUNKS)]
    token_copies = {}
    for which, k in order:
        if (which, k) == (1, 0):
            for i in range(3):
                pick_copy(i).start()
        for route in (1, 0):
            token_copy(which, k, route).start()

    def picked(slot):
        held = pick_in[...] if slot == 0 else picks[slot - 1]
        lane = lax.broadcasted_iota(jnp.int32, held.shape, 1)
        return jnp.sum(jnp.where(lane == e, held.astype(jnp.float32), 0.0), axis=1, keepdims=True)

    def forward_x(slot):
        rows = pl.ds(slot * tok, tok)
        both_s[rows, :] = jnp.dot(xs[slot], wgu[...], preferred_element_type=jnp.float32) * (1.0 / math.sqrt(width))

    def turn_x(slot):
        span = 512
        for at in range(0, width, span):
            xt[pl.ds(at, span), pl.ds(slot * tok, tok)] = xs[slot, :, at:at + span].T

    def activate(slot):
        rows = pl.ds(slot * tok, tok)
        gate, upper = both_s[rows, :hid], both_s[rows, hid:]
        act = gate * jax.nn.sigmoid(gate) * upper * picked(slot)
        act_s[:, rows] = act.T.astype(jnp.bfloat16)

    def backward(slot):
        rows = pl.ds(slot * tok, tok)
        gate, upper = both_s[rows, :hid], both_s[rows, hid:]
        sigma = jax.nn.sigmoid(gate)
        dact = lax.dot_general(dys[slot], wdown[...], (((1,), (1,)), ((), ())), preferred_element_type=jnp.float32)
        dact = dact * (1.0 / math.sqrt(hid)) * picked(slot)
        dgu_s[rows, :hid] = (dact * upper * sigma * (1.0 + gate * (1.0 - sigma))).astype(jnp.bfloat16)
        dgu_s[rows, hid:] = (dact * gate * sigma).astype(jnp.bfloat16)

    gu_rows, down_rows = width // nodes, hid // nodes
    gu_part, down_part = gu_rows // GU_CHUNKS, width // DOWN_CHUNKS
    chunks = [("down", j) for j in range(DOWN_CHUNKS)] + [("gu", c) for c in range(GU_CHUNKS)]

    def piece_of(kind, c, ref, owner):
        if kind == "gu":
            return ref.at[pl.ds(owner * gu_rows + c * gu_part, gu_part), :]
        return ref.at[pl.ds(owner * down_rows, down_rows), pl.ds(c * down_part, down_part)]

    def places(phase, kind, c):
        p, l, m, og = (p_gu, l_gu, m_gu, og_gu) if kind == "gu" else (p_down, l_down, m_down, og_down)
        if phase == 0:
            return (lambda to: piece_of(kind, c, p, to)), (lambda of: l.at[c, of])
        return (lambda to: m.at[c, to]), (lambda of: piece_of(kind, c, og, of))

    relayed = (deep // 2, 1)

    def send(phase, kind, c, i):
        dz, dx = offsets[i]
        source, lands = places(phase, kind, c)
        at = phase * len(chunks) + chunks.index((kind, c))
        to = node_at(dz, dx)
        via, dst = to, lands(me)
        if (dz, dx) == relayed:
            via = node_at(-1, 0)
            dst = (t_gu if kind == "gu" else t_down).at[phase, c]
        return pltpu.make_async_remote_copy(
            source(to), dst, a_send.at[at, i], a_recv.at[at, i], device_id={"node": via}, device_id_type=MESH)

    def pass_on(phase, kind, c):
        at = phase * len(chunks) + chunks.index((kind, c))
        lands = places(phase, kind, c)[1]
        return pltpu.make_async_remote_copy(
            (t_gu if kind == "gu" else t_down).at[phase, c], lands(node_at(1, 0)),
            a_send.at[at, len(offsets)], a_recv.at[at, len(offsets)],
            device_id={"node": node_at(relayed[0] + 1, relayed[1])}, device_id_type=MESH)

    first = [offsets.index(relayed)] + [i for i, o in enumerate(offsets) if o != relayed]

    def send_all(phase, kind, c):
        for i in first:
            send(phase, kind, c, i).start()

    def relay(phase, kind, c):
        send(phase, kind, c, first[0]).wait_recv()
        pass_on(phase, kind, c).start()

    def arrived(phase, kind, c):
        for i in first[1:]:
            send(phase, kind, c, i).wait_recv()
        pass_on(phase, kind, c).wait_recv()

    def sent(phase, kind, c):
        for i in first:
            send(phase, kind, c, i).wait_send()
        pass_on(phase, kind, c).wait_send()

    def mix_block(parts):
        total = parts[0]
        for part in parts[1:]:
            total = total + part
        mixed = []
        for to in range(nodes):
            acc = parts[0] * mix_ref[to, 0]
            for of in range(1, nodes):
                acc = acc + parts[of] * mix_ref[to, of]
            mixed.append(acc.astype(jnp.bfloat16))
        return total * (1.0 / nodes), mixed

    def own(kind, c):
        if kind == "gu":
            return pltpu.make_async_copy(m_gu.at[c, me], piece_of(kind, c, og_gu, me), loc_sem.at[4 + c])
        return pltpu.make_async_copy(m_down.at[c, me], piece_of(kind, c, og_down, me), loc_sem.at[4 + GU_CHUNKS + c])

    def mix(kind, c):
        if kind == "gu":
            tall, wide = math.gcd(32, gu_part), 128

            def step(b, carry):
                rows = pl.ds(pl.multiple_of(b * tall, tall), tall)
                for at in range(0, 2 * hid, wide):
                    parts = [l_gu[c, of, rows, at:at + wide].astype(jnp.float32) for of in range(nodes)]
                    mean, mixed = mix_block(parts)
                    avg_gu[pl.ds(pl.multiple_of(c * gu_part + b * tall, tall), tall), at:at + wide] = mean
                    for to in range(nodes):
                        m_gu[c, to, rows, at:at + wide] = mixed[to]
                return carry
            lax.fori_loop(0, gu_part // tall, step, 0)
        else:
            wide = 256

            def step(b, carry):
                cols = pl.ds(pl.multiple_of(b * wide, wide), wide)
                parts = [l_down[c, of, :, cols].astype(jnp.float32) for of in range(nodes)]
                mean, mixed = mix_block(parts)
                avg_down[:, pl.ds(pl.multiple_of(c * down_part + b * wide, wide), wide)] = mean
                for to in range(nodes):
                    m_down[c, to, :, cols] = mixed[to]
                return carry
            lax.fori_loop(0, down_part // wide, step, 0)

    def finish(kind, c):
        arrived(0, kind, c)
        mix(kind, c)
        send_all(1, kind, c)
        own(kind, c).start()

    local[1].wait()
    wgu[...] = par_gu[...].astype(jnp.bfloat16)
    local[2].wait()
    wdown[...] = par_down[...].astype(jnp.bfloat16)
    local[0].wait()
    forward_x(0)
    turn_x(0)
    for k in range(X_CHUNKS):
        token_copy(0, k, 0).wait_recv()
    forward_x(1)
    local[3].wait()
    for k in range(X_CHUNKS):
        token_copy(0, k, 1).wait_recv()
        token_copy(0, k, 2).start()
        if k == 0:
            turn_x(1)
    for i in range(3):
        pick_copy(i).wait_recv()
    forward_x(2)
    for slot in range(3):
        activate(slot)
    for k in range(X_CHUNKS):
        token_copy(0, k, 2).wait_recv()
    forward_x(3)
    activate(3)
    per_down = DY_CHUNKS // DOWN_CHUNKS
    for k in range(DY_CHUNKS):
        token_copy(1, k, 0).wait_recv()
        token_copy(1, k, 1).wait_recv()
        token_copy(1, k, 2).start()
        if k == 0:
            backward(0)
            turn_x(2)
        if k == 1:
            turn_x(3)
        token_copy(1, k, 2).wait_recv()
        size = width // DY_CHUNKS
        cols = slice(k * size, (k + 1) * size)
        grad = jnp.dot(act_s[:, :tok], dys[0, :, cols], preferred_element_type=jnp.float32)
        for slot in range(1, 4):
            grad = grad + jnp.dot(act_s[:, slot * tok:(slot + 1) * tok], dys[slot, :, cols], preferred_element_type=jnp.float32)
        p_down[:, cols] = (par_down[:, cols] - grad * (0.5 / math.sqrt(hid))).astype(jnp.bfloat16)
        if k % per_down == per_down - 1:
            j = k // per_down
            span = pl.ds(j * down_part, down_part)
            l_down[j, me] = p_down[pl.ds(pl.multiple_of(me * down_rows, down_rows), down_rows), span]
            send_all(0, "down", j)
    for slot in range(1, 4):
        backward(slot)
    relay(0, "down", 0)

    for c in range(GU_CHUNKS):
        def grad_part(m, carry):
            rows = pl.ds(pl.multiple_of(m * gu_rows + c * gu_part, gu_part), gu_part)
            grad = jnp.dot(xt[rows, :], dgu_s[...], preferred_element_type=jnp.float32)
            p_gu[rows, :] = (par_gu[rows, :] - grad * (0.5 / math.sqrt(width))).astype(jnp.bfloat16)
            return carry
        lax.fori_loop(0, nodes, grad_part, 0)
        l_gu[c, me] = p_gu[pl.ds(pl.multiple_of(me * gu_rows + c * gu_part, gu_part), gu_part), :]
        send_all(0, "gu", c)
        if c == 0:
            relay(0, "down", 1)
            finish("down", 0)
    relay(0, "gu", 0)
    finish("down", 1)
    queue = [("gu", c) for c in range(GU_CHUNKS)]
    for c in range(GU_CHUNKS):
        if c + 1 < GU_CHUNKS:
            relay(0, "gu", c + 1)
        finish("gu", c)
        if c < DOWN_CHUNKS:
            relay(1, "down", c)
        else:
            relay(1, "gu", c - DOWN_CHUNKS)
    for c in range(GU_CHUNKS - DOWN_CHUNKS, GU_CHUNKS):
        relay(1, "gu", c)
    for kind, c in chunks:
        arrived(1, kind, c)
        own(kind, c).wait()
    for kind, c in chunks:
        sent(0, kind, c)
        sent(1, kind, c)
    for which, k in order:
        for route in range(3):
            token_copy(which, k, route).wait_send()
    for i in range(3):
        pick_copy(i).wait_send()


def body(param_gu, param_down, tokens, cotangent, routes, plan):
    nodes = lax.axis_size("node")
    groups = lax.axis_size("expert")
    tok, width = tokens.shape
    hid = param_down.shape[0]
    rows = hid // nodes
    if groups != 4 or nodes % 4 or rows % 16 or (width // nodes) % (16 * GU_CHUNKS):
        return plain_body(param_gu, param_down, tokens, cotangent, routes, plan)
    mixing = mixing_of(plan, nodes)
    pick = jnp.any(routes[:, :, None] == jnp.arange(128, dtype=jnp.int32), axis=1).astype(jnp.bfloat16)
    bf, f32 = jnp.bfloat16, jnp.float32
    gu_part, down_part = width // nodes // GU_CHUNKS, width // DOWN_CHUNKS
    n_chunks = GU_CHUNKS + DOWN_CHUNKS
    anywhere = pl.BlockSpec(memory_space=pl.ANY)
    vmem = pl.BlockSpec(memory_space=pltpu.VMEM)
    return pl.pallas_call(
        partial(kernel, nodes),
        out_shape=(
            jax.ShapeDtypeStruct(param_gu.shape, bf), jax.ShapeDtypeStruct(param_down.shape, bf),
            jax.ShapeDtypeStruct((width // nodes, 2 * hid), f32), jax.ShapeDtypeStruct((rows, width), f32)),
        in_specs=[pl.BlockSpec(memory_space=pltpu.SMEM), anywhere, anywhere, anywhere, anywhere, vmem],
        out_specs=(anywhere, anywhere, vmem, vmem),
        scratch_shapes=[
            pltpu.VMEM(param_gu.shape, f32), pltpu.VMEM(param_down.shape, f32),
            pltpu.VMEM((4, tok, width), bf), pltpu.VMEM((4, tok, width), bf), pltpu.VMEM((width, 4 * tok), bf),
            pltpu.VMEM((3, tok, 128), bf), pltpu.VMEM(param_gu.shape, bf), pltpu.VMEM(param_down.shape, bf),
            pltpu.VMEM((4 * tok, 2 * hid), f32), pltpu.VMEM((hid, 4 * tok), bf), pltpu.VMEM((4 * tok, 2 * hid), bf),
            pltpu.VMEM(param_gu.shape, bf), pltpu.VMEM(param_down.shape, bf),
            pltpu.VMEM((GU_CHUNKS, nodes, gu_part, 2 * hid), bf), pltpu.VMEM((DOWN_CHUNKS, nodes, rows, down_part), bf),
            pltpu.VMEM((2, GU_CHUNKS, gu_part, 2 * hid), bf), pltpu.VMEM((2, DOWN_CHUNKS, rows, down_part), bf),
            pltpu.VMEM((GU_CHUNKS, nodes, gu_part, 2 * hid), bf), pltpu.VMEM((DOWN_CHUNKS, nodes, rows, down_part), bf),
            pltpu.SemaphoreType.DMA((4 + n_chunks,)),
            pltpu.SemaphoreType.DMA((X_CHUNKS + DY_CHUNKS, 3)), pltpu.SemaphoreType.DMA((X_CHUNKS + DY_CHUNKS, 3)),
            pltpu.SemaphoreType.DMA((3,)), pltpu.SemaphoreType.DMA((3,)),
            pltpu.SemaphoreType.DMA((2 * n_chunks, nodes)), pltpu.SemaphoreType.DMA((2 * n_chunks, nodes)),
        ],
        compiler_params=pltpu.CompilerParams(collective_id=1, has_side_effects=True, vmem_limit_bytes=60 * 2**20),
    )(mixing, param_gu, param_down, tokens, cotangent, pick)


def solution(mesh):
    both = P("node", "expert")
    rows = P(("node", "expert"), None)
    return jax.shard_map(body, mesh=mesh, in_specs=(both, both, rows, rows, rows, P()), out_specs=(both,) * 4, check_vma=False)
```

```python
from functools import partial
import math

import jax
import jax.numpy as jnp
from jax import lax
from jax.experimental import pallas as pl
from jax.experimental.pallas import tpu as pltpu
from jax.sharding import PartitionSpec as P


def everyone(value, axis):
    count = lax.axis_size(axis)
    spread = jnp.broadcast_to(value[None], (count,) + value.shape)
    return lax.all_to_all(spread, axis, 0, 0)


def plain_body(param_gu, param_down, tokens, cotangent, routes, plan):
    nodes = lax.axis_size("node")
    width = tokens.shape[1]
    hid = param_down.shape[0]
    mine = lax.axis_index("expert")
    rows = everyone(tokens, "expert").reshape(-1, width)
    douts = everyone(cotangent, "expert").reshape(-1, width)
    chosen = lax.all_gather(routes, "expert", axis=0, tiled=True)
    picked = jnp.any(chosen == mine, axis=1)[:, None]
    wgu = param_gu.astype(jnp.bfloat16)
    wdown = param_down.astype(jnp.bfloat16)
    both = jnp.dot(rows, wgu, preferred_element_type=jnp.float32) * (1.0 / math.sqrt(width))
    gate = both[:, :hid]
    upper = both[:, hid:]
    sigma = jax.nn.sigmoid(gate)
    act = jnp.where(picked, gate * sigma * upper, 0.0).astype(jnp.bfloat16)
    dact = jnp.dot(douts, wdown.T, preferred_element_type=jnp.float32) * (1.0 / math.sqrt(hid))
    dgate = dact * upper * sigma * (1.0 + gate * (1.0 - sigma))
    dupper = dact * gate * sigma
    dboth = jnp.where(picked, jnp.concatenate([dgate, dupper], axis=1), 0.0).astype(jnp.bfloat16)
    grad_down = jnp.dot(act.T, douts, preferred_element_type=jnp.float32) * (1.0 / math.sqrt(hid))
    grad_gu = jnp.dot(rows.T, dboth, preferred_element_type=jnp.float32) * (1.0 / math.sqrt(width))
    state_gu = (param_gu - 0.5 * grad_gu).astype(jnp.bfloat16)
    state_down = (param_down - 0.5 * grad_down).astype(jnp.bfloat16)

    distance = jnp.left_shift(jnp.int32(1), plan) % nodes
    ranks = jnp.arange(nodes)
    mixing = jnp.eye(nodes, dtype=jnp.float32)
    for step in range(plan.shape[0]):
        mixing = 0.5 * (mixing + jnp.take(mixing, (ranks + distance[step]) % nodes, axis=0))

    def gossip(state):
        split = state.reshape(nodes, -1, state.shape[1])
        held = lax.all_to_all(split, "node", 0, 0)
        mean = jnp.mean(held.astype(jnp.float32), axis=0)
        mixed = jnp.einsum("nm,mrc->nrc", mixing.astype(jnp.bfloat16), held, preferred_element_type=jnp.float32)
        back = lax.all_to_all(mixed.astype(jnp.bfloat16), "node", 0, 0)
        return back.reshape(state.shape), mean

    gossiped_down, averaged_down = gossip(state_down)
    gossiped_gu, averaged_gu = gossip(state_gu)
    return (gossiped_gu, gossiped_down, averaged_gu, averaged_down)


X_CHUNKS = 2
DY_CHUNKS = 4
GU_CHUNKS = 4
DOWN_CHUNKS = 2
MESH = pl.DeviceIdType.MESH


def mixing_of(plan, nodes):
    rounds = plan.shape[0]
    ranks = jnp.arange(nodes)
    distance = jnp.left_shift(jnp.int32(1), plan) % nodes
    taken = (jnp.arange(2**rounds)[:, None] >> jnp.arange(rounds)[None, :]) & 1
    reach = jnp.sum(taken * distance[None, :], axis=1)
    hits = (ranks[:, None, None] + reach) % nodes == ranks[None, :, None]
    return jnp.mean(hits.astype(jnp.float32), axis=2)


def kernel(nodes, mix_ref, gu_in, down_in, x_in, dy_in, pick_in, og_gu, og_down, avg_gu, avg_down,
           par_gu, par_down, xs, dys, xt, picks, wgu, wdown, both_s, act_s, dgu_s,
           p_gu, p_down, l_gu, l_down, t_gu, t_down, m_gu, m_down,
           loc_sem, tok_send, tok_recv, pick_send, pick_recv, a_send, a_recv):
    me = lax.axis_index("node")
    e = lax.axis_index("expert")
    deep = nodes // 2
    z, x = lax.div(me, 2), lax.rem(me, 2)
    partner = e + 1 - 2 * lax.rem(e, 2)
    cross = lax.rem(e + 2, 4)
    diag = partner + 2 - 4 * lax.div(partner, 2)
    tok, width = x_in.shape
    hid = down_in.shape[0]

    def node_at(dz, dx):
        return lax.rem(z + dz + deep, deep) * 2 + lax.rem(x + dx, 2)

    barrier = pltpu.get_barrier_semaphore()
    offsets = [(dz, dx) for dz in range(deep) for dx in range(2)][1:]
    for other in (partner, cross, diag):
        pl.semaphore_signal(barrier, inc=1, device_id={"expert": other}, device_id_type=MESH)
    for dz, dx in offsets:
        pl.semaphore_signal(barrier, inc=1, device_id={"node": node_at(dz, dx)}, device_id_type=MESH)

    local = [
        pltpu.make_async_copy(x_in, xs.at[0], loc_sem.at[0]),
        pltpu.make_async_copy(gu_in, par_gu, loc_sem.at[1]),
        pltpu.make_async_copy(down_in, par_down, loc_sem.at[2]),
        pltpu.make_async_copy(dy_in, dys.at[0], loc_sem.at[3]),
    ]
    for copy in local:
        copy.start()
    pl.semaphore_wait(barrier, 3 + len(offsets))

    def piece(which, k):
        if which == 0:
            size = tok // X_CHUNKS
            return (pl.ds(k * size, size), slice(None))
        size = width // DY_CHUNKS
        return (slice(None), pl.ds(k * size, size))

    def token_copy(which, k, route):
        part = piece(which, k)
        buf = (xs, dys)[which]
        at = (0 if which == 0 else X_CHUNKS) + k
        if route == 2:
            src = buf.at[(2,) + part]
        else:
            src = (x_in, dy_in)[which].at[part]
        return pltpu.make_async_remote_copy(
            src, buf.at[(route + 1,) + part], tok_send.at[at, route], tok_recv.at[at, route],
            device_id={"expert": cross if route == 1 else partner}, device_id_type=MESH)

    def pick_copy(i):
        return pltpu.make_async_remote_copy(
            pick_in, picks.at[i], pick_send.at[i], pick_recv.at[i],
            device_id={"expert": (partner, cross, diag)[i]}, device_id_type=MESH)

    order = [(0, k) for k in range(X_CHUNKS)] + [(1, k) for k in range(DY_CHUNKS)]
    token_copies = {}
    for which, k in order:
        if (which, k) == (1, 0):
            for i in range(3):
                pick_copy(i).start()
        for route in (1, 0):
            token_copy(which, k, route).start()

    def picked(slot):
        held = pick_in[...] if slot == 0 else picks[slot - 1]
        lane = lax.broadcasted_iota(jnp.int32, held.shape, 1)
        return jnp.sum(jnp.where(lane == e, held.astype(jnp.float32), 0.0), axis=1, keepdims=True)

    def forward_x(slot):
        rows = pl.ds(slot * tok, tok)
        both_s[rows, :] = jnp.dot(xs[slot], wgu[...], preferred_element_type=jnp.float32) * (1.0 / math.sqrt(width))

    def turn_x(slot):
        span = 512
        for at in range(0, width, span):
            xt[pl.ds(at, span), pl.ds(slot * tok, tok)] = xs[slot, :, at:at + span].T

    def activate(slot):
        rows = pl.ds(slot * tok, tok)
        gate, upper = both_s[rows, :hid], both_s[rows, hid:]
        act = gate * jax.nn.sigmoid(gate) * upper * picked(slot)
        act_s[:, rows] = act.T.astype(jnp.bfloat16)

    def backward(slot):
        rows = pl.ds(slot * tok, tok)
        gate, upper = both_s[rows, :hid], both_s[rows, hid:]
        sigma = jax.nn.sigmoid(gate)
        dact = lax.dot_general(dys[slot], wdown[...], (((1,), (1,)), ((), ())), preferred_element_type=jnp.float32)
        dact = dact * (1.0 / math.sqrt(hid)) * picked(slot)
        dgu_s[rows, :hid] = (dact * upper * sigma * (1.0 + gate * (1.0 - sigma))).astype(jnp.bfloat16)
        dgu_s[rows, hid:] = (dact * gate * sigma).astype(jnp.bfloat16)

    gu_rows, down_rows = width // nodes, hid // nodes
    gu_part, down_part = gu_rows // GU_CHUNKS, width // DOWN_CHUNKS
    chunks = [("down", j) for j in range(DOWN_CHUNKS)] + [("gu", c) for c in range(GU_CHUNKS)]

    def piece_of(kind, c, ref, owner):
        if kind == "gu":
            return ref.at[pl.ds(owner * gu_rows + c * gu_part, gu_part), :]
        return ref.at[pl.ds(owner * down_rows, down_rows), pl.ds(c * down_part, down_part)]

    def places(phase, kind, c):
        p, l, m, og = (p_gu, l_gu, m_gu, og_gu) if kind == "gu" else (p_down, l_down, m_down, og_down)
        if phase == 0:
            return (lambda to: piece_of(kind, c, p, to)), (lambda of: l.at[c, of])
        return (lambda to: m.at[c, to]), (lambda of: piece_of(kind, c, og, of))

    relayed = (deep // 2, 1)

    def send(phase, kind, c, i):
        dz, dx = offsets[i]
        source, lands = places(phase, kind, c)
        at = phase * len(chunks) + chunks.index((kind, c))
        to = node_at(dz, dx)
        via, dst = to, lands(me)
        if (dz, dx) == relayed:
            via = node_at(-1, 0)
            dst = (t_gu if kind == "gu" else t_down).at[phase, c]
        return pltpu.make_async_remote_copy(
            source(to), dst, a_send.at[at, i], a_recv.at[at, i], device_id={"node": via}, device_id_type=MESH)

    def pass_on(phase, kind, c):
        at = phase * len(chunks) + chunks.index((kind, c))
        lands = places(phase, kind, c)[1]
        return pltpu.make_async_remote_copy(
            (t_gu if kind == "gu" else t_down).at[phase, c], lands(node_at(1, 0)),
            a_send.at[at, len(offsets)], a_recv.at[at, len(offsets)],
            device_id={"node": node_at(relayed[0] + 1, relayed[1])}, device_id_type=MESH)

    first = [offsets.index(relayed)] + [i for i, o in enumerate(offsets) if o != relayed]

    def send_all(phase, kind, c):
        for i in first:
            send(phase, kind, c, i).start()

    def relay(phase, kind, c):
        send(phase, kind, c, first[0]).wait_recv()
        pass_on(phase, kind, c).start()

    def arrived(phase, kind, c):
        for i in first[1:]:
            send(phase, kind, c, i).wait_recv()
        pass_on(phase, kind, c).wait_recv()

    def sent(phase, kind, c):
        for i in first:
            send(phase, kind, c, i).wait_send()
        pass_on(phase, kind, c).wait_send()

    def mix_block(parts):
        total = parts[0]
        for part in parts[1:]:
            total = total + part
        mixed = []
        for to in range(nodes):
            acc = parts[0] * mix_ref[to, 0]
            for of in range(1, nodes):
                acc = acc + parts[of] * mix_ref[to, of]
            mixed.append(acc.astype(jnp.bfloat16))
        return total * (1.0 / nodes), mixed

    def own(kind, c):
        if kind == "gu":
            return pltpu.make_async_copy(m_gu.at[c, me], piece_of(kind, c, og_gu, me), loc_sem.at[4 + c])
        return pltpu.make_async_copy(m_down.at[c, me], piece_of(kind, c, og_down, me), loc_sem.at[4 + GU_CHUNKS + c])

    def mix(kind, c):
        if kind == "gu":
            tall, wide = math.gcd(32, gu_part), 128

            def step(b, carry):
                rows = pl.ds(pl.multiple_of(b * tall, tall), tall)
                for at in range(0, 2 * hid, wide):
                    parts = [l_gu[c, of, rows, at:at + wide].astype(jnp.float32) for of in range(nodes)]
                    mean, mixed = mix_block(parts)
                    avg_gu[pl.ds(pl.multiple_of(c * gu_part + b * tall, tall), tall), at:at + wide] = mean
                    for to in range(nodes):
                        m_gu[c, to, rows, at:at + wide] = mixed[to]
                return carry
            lax.fori_loop(0, gu_part // tall, step, 0)
        else:
            wide = 256

            def step(b, carry):
                cols = pl.ds(pl.multiple_of(b * wide, wide), wide)
                parts = [l_down[c, of, :, cols].astype(jnp.float32) for of in range(nodes)]
                mean, mixed = mix_block(parts)
                avg_down[:, pl.ds(pl.multiple_of(c * down_part + b * wide, wide), wide)] = mean
                for to in range(nodes):
                    m_down[c, to, :, cols] = mixed[to]
                return carry
            lax.fori_loop(0, down_part // wide, step, 0)

    def finish(kind, c):
        arrived(0, kind, c)
        mix(kind, c)
        send_all(1, kind, c)
        own(kind, c).start()

    local[1].wait()
    wgu[...] = par_gu[...].astype(jnp.bfloat16)
    local[2].wait()
    wdown[...] = par_down[...].astype(jnp.bfloat16)
    local[0].wait()
    forward_x(0)
    turn_x(0)
    for k in range(X_CHUNKS):
        token_copy(0, k, 0).wait_recv()
    forward_x(1)
    local[3].wait()
    for k in range(X_CHUNKS):
        token_copy(0, k, 1).wait_recv()
        token_copy(0, k, 2).start()
        if k == 0:
            turn_x(1)
    for i in range(3):
        pick_copy(i).wait_recv()
    forward_x(2)
    for slot in range(3):
        activate(slot)
    for k in range(X_CHUNKS):
        token_copy(0, k, 2).wait_recv()
    forward_x(3)
    activate(3)
    per_down = DY_CHUNKS // DOWN_CHUNKS
    for k in range(DY_CHUNKS):
        token_copy(1, k, 0).wait_recv()
        token_copy(1, k, 1).wait_recv()
        token_copy(1, k, 2).start()
        if k == 0:
            backward(0)
            turn_x(2)
        if k == 1:
            turn_x(3)
        token_copy(1, k, 2).wait_recv()
        size = width // DY_CHUNKS
        cols = slice(k * size, (k + 1) * size)
        grad = jnp.dot(act_s[:, :tok], dys[0, :, cols], preferred_element_type=jnp.float32)
        for slot in range(1, 4):
            grad = grad + jnp.dot(act_s[:, slot * tok:(slot + 1) * tok], dys[slot, :, cols], preferred_element_type=jnp.float32)
        p_down[:, cols] = (par_down[:, cols] - grad * (0.5 / math.sqrt(hid))).astype(jnp.bfloat16)
        if k % per_down == per_down - 1:
            j = k // per_down
            span = pl.ds(j * down_part, down_part)
            l_down[j, me] = p_down[pl.ds(pl.multiple_of(me * down_rows, down_rows), down_rows), span]
            send_all(0, "down", j)
    for slot in range(1, 4):
        backward(slot)
    relay(0, "down", 0)

    for c in range(GU_CHUNKS):
        def grad_part(m, carry):
            rows = pl.ds(pl.multiple_of(m * gu_rows + c * gu_part, gu_part), gu_part)
            grad = jnp.dot(xt[rows, :], dgu_s[...], preferred_element_type=jnp.float32)
            p_gu[rows, :] = (par_gu[rows, :] - grad * (0.5 / math.sqrt(width))).astype(jnp.bfloat16)
            return carry
        lax.fori_loop(0, nodes, grad_part, 0)
        l_gu[c, me] = p_gu[pl.ds(pl.multiple_of(me * gu_rows + c * gu_part, gu_part), gu_part), :]
        send_all(0, "gu", c)
        if c == 0:
            relay(0, "down", 1)
            finish("down", 0)
    finish("down", 1)
    for c in range(GU_CHUNKS):
        relay(0, "gu", c)
    for j in range(DOWN_CHUNKS):
        relay(1, "down", j)
    for c in range(GU_CHUNKS):
        finish("gu", c)
        if c:
            relay(1, "gu", c - 1)
    relay(1, "gu", GU_CHUNKS - 1)
    for kind, c in chunks:
        arrived(1, kind, c)
        own(kind, c).wait()
    for kind, c in chunks:
        sent(0, kind, c)
        sent(1, kind, c)
    for which, k in order:
        for route in range(3):
            token_copy(which, k, route).wait_send()
    for i in range(3):
        pick_copy(i).wait_send()


def body(param_gu, param_down, tokens, cotangent, routes, plan):
    nodes = lax.axis_size("node")
    groups = lax.axis_size("expert")
    tok, width = tokens.shape
    hid = param_down.shape[0]
    rows = hid // nodes
    if groups != 4 or nodes % 4 or rows % 16 or (width // nodes) % (16 * GU_CHUNKS):
        return plain_body(param_gu, param_down, tokens, cotangent, routes, plan)
    mixing = mixing_of(plan, nodes)
    pick = jnp.any(routes[:, :, None] == jnp.arange(128, dtype=jnp.int32), axis=1).astype(jnp.bfloat16)
    bf, f32 = jnp.bfloat16, jnp.float32
    gu_part, down_part = width // nodes // GU_CHUNKS, width // DOWN_CHUNKS
    n_chunks = GU_CHUNKS + DOWN_CHUNKS
    anywhere = pl.BlockSpec(memory_space=pl.ANY)
    vmem = pl.BlockSpec(memory_space=pltpu.VMEM)
    return pl.pallas_call(
        partial(kernel, nodes),
        out_shape=(
            jax.ShapeDtypeStruct(param_gu.shape, bf), jax.ShapeDtypeStruct(param_down.shape, bf),
            jax.ShapeDtypeStruct((width // nodes, 2 * hid), f32), jax.ShapeDtypeStruct((rows, width), f32)),
        in_specs=[pl.BlockSpec(memory_space=pltpu.SMEM), anywhere, anywhere, anywhere, anywhere, vmem],
        out_specs=(anywhere, anywhere, vmem, vmem),
        scratch_shapes=[
            pltpu.VMEM(param_gu.shape, f32), pltpu.VMEM(param_down.shape, f32),
            pltpu.VMEM((4, tok, width), bf), pltpu.VMEM((4, tok, width), bf), pltpu.VMEM((width, 4 * tok), bf),
            pltpu.VMEM((3, tok, 128), bf), pltpu.VMEM(param_gu.shape, bf), pltpu.VMEM(param_down.shape, bf),
            pltpu.VMEM((4 * tok, 2 * hid), f32), pltpu.VMEM((hid, 4 * tok), bf), pltpu.VMEM((4 * tok, 2 * hid), bf),
            pltpu.VMEM(param_gu.shape, bf), pltpu.VMEM(param_down.shape, bf),
            pltpu.VMEM((GU_CHUNKS, nodes, gu_part, 2 * hid), bf), pltpu.VMEM((DOWN_CHUNKS, nodes, rows, down_part), bf),
            pltpu.VMEM((2, GU_CHUNKS, gu_part, 2 * hid), bf), pltpu.VMEM((2, DOWN_CHUNKS, rows, down_part), bf),
            pltpu.VMEM((GU_CHUNKS, nodes, gu_part, 2 * hid), bf), pltpu.VMEM((DOWN_CHUNKS, nodes, rows, down_part), bf),
            pltpu.SemaphoreType.DMA((4 + n_chunks,)),
            pltpu.SemaphoreType.DMA((X_CHUNKS + DY_CHUNKS, 3)), pltpu.SemaphoreType.DMA((X_CHUNKS + DY_CHUNKS, 3)),
            pltpu.SemaphoreType.DMA((3,)), pltpu.SemaphoreType.DMA((3,)),
            pltpu.SemaphoreType.DMA((2 * n_chunks, nodes)), pltpu.SemaphoreType.DMA((2 * n_chunks, nodes)),
        ],
        compiler_params=pltpu.CompilerParams(collective_id=1, has_side_effects=True, vmem_limit_bytes=60 * 2**20),
    )(mixing, param_gu, param_down, tokens, cotangent, pick)


def solution(mesh):
    both = P("node", "expert")
    rows = P(("node", "expert"), None)
    return jax.shard_map(body, mesh=mesh, in_specs=(both, both, rows, rows, rows, P()), out_specs=(both,) * 4, check_vma=False)
```
